32 devices in a mesh: dp: 2 (over x), expert: 8 (over z, y), tensor: 2 (over core).
Axes of the slice: x: 2, y: 2, z: 4, core: 2. Of those that a mesh axis runs over, the one named last changes fastest.
Arguments:
- tokens: bfloat16 [2048, 2048], P(('dp', 'expert')), may hold values from -6 to 6
- norm_gain: float32 [2048], replicated, may hold values from 0.1 to 1.9
- router: bfloat16 [2048, 8], replicated, may hold values from -0.125 to 0.125
- expert_ids: int32 [2048, 4], P(('dp', 'expert')), may hold values from 0 to 7, all different within a row; in each aligned block of 128 rows (0 to 127, 128 to 255, ...) at most 80 rows name the same one
- modality: int32 [2048], P(('dp', 'expert')), may hold values from 0 to 1, as said below
- expert_gate: bfloat16 [8, 2048, 1408], P('expert', None, 'tensor'), may hold values from -0.125 to 0.125
- expert_up: bfloat16 [8, 2048, 1408], P('expert', None, 'tensor'), may hold values from -0.125 to 0.125
- expert_down: bfloat16 [8, 1408, 2048], P('expert', 'tensor'), may hold values from -0.15625 to 0.15625
- shared_gate: bfloat16 [2, 2048, 704], P(None, None, ('dp', 'tensor')), may hold values from -0.125 to 0.125
- shared_up: bfloat16 [2, 2048, 704], P(None, None, ('dp', 'tensor')), may hold values from -0.125 to 0.125
- shared_down: bfloat16 [2, 704, 2048], P(None, ('dp', 'tensor')), may hold values from -0.21875 to 0.21875
Outputs:
- mixed: bfloat16 [2048, 2048], P(('dp', 'expert'), 'tensor')
The draws below stay inside these ranges and needn't reach their ends.
Inputs may be any that keep to these rules, and one draw needn't show every extreme that they name: `expert_ids`: each token names 4 different experts; among the 128 tokens of one device (aligned blocks of rows) no expert is named by more than 80 tokens, and some expert reaches 80. `modality`: within each aligned block of 128 tokens the image patches form one run (taken cyclically) that covers from an eighth to seven eighths of the block.
All inputs are finite; a program needn't handle non-finite values.
Results may differ from the reference program's by a relative error of at most 0.0073.
Values may be sent and summed in bfloat16 or wider, within the bound.
No kernel may reach another device: no remote copies, remote signals or barrier semaphores. Data moves between devices by JAX's collectives and lax.ppermute only.
A program may use at most 128 MiB of HBM per device.

```python
import math
import jax
import jax.numpy as jnp
import numpy as np
from jax import lax

D = 2048
FF = 1408
SH = 704
TOP = 4
TOK_DEV = 128
EXPERTS = 8
TOKENS = 2048
CAP = 80


def draw_modality(key, part):
    blocks = TOKENS // TOK_DEV
    share_key, start_key = jax.random.split(jax.random.fold_in(key, 11))
    counts = jax.random.randint(share_key, (blocks, 1), TOK_DEV // 8, TOK_DEV - TOK_DEV // 8 + 1)
    starts = jax.random.randint(start_key, (blocks, 1), 0, TOK_DEV)
    position = jnp.arange(TOK_DEV, dtype=jnp.int32)[None, :]
    image_flags = ((position - starts) % TOK_DEV < counts).astype(jnp.int32)
    return image_flags.reshape(-1)


def steps_of(stream_key, shape, pieces, smallest, high):
    loudness, own = 1.0, jax.random.fold_in(stream_key, 6)
    for dim, blocks in pieces:
        draws = jnp.exp(jax.random.uniform(jax.random.fold_in(own, dim), (blocks,), jnp.float32, smallest / len(pieces), high / len(pieces)))
        loudness = loudness * jnp.repeat(draws, shape[dim] // blocks).reshape([-1 if axis == dim else 1 for axis in range(len(shape))])
    return loudness


def deal_out(rng, own, number, rows, amount, top, bound, slope):
    ranking = jax.random.permutation(rng, amount)
    heavy_load, usual = portions_of(amount, rows * top, bound, slope, True), portions_of(amount, rows * top, bound, slope, False)
    places = jnp.arange(amount)

    def named(tallies, rotation):
        used = int((tallies > 0).sum())
        fixed = max(1, used // 4)
        passed = fixed + (places - fixed + rotation * (used - fixed)) % max(1, amount - fixed)
        return jnp.zeros((amount,), jnp.int32).at[ranking[jnp.where(places < fixed, places, passed)]].set(jnp.asarray(tallies, jnp.int32))

    tallies = jnp.where(number % 4 == 0, named(heavy_load, number // 4), named(usual, number - number // 4 - 1))
    mixed = jax.random.permutation(jax.random.fold_in(own, 3), amount)
    giver, sink = mixed[0:amount // 2 * 2:2], mixed[1:amount // 2 * 2:2]
    margin = jnp.minimum(tallies[giver] - 1, bound - tallies[sink]) // 2
    margin = jnp.where((giver == ranking[0]) | (sink == ranking[0]) | (tallies[sink] == 0), 0, jnp.maximum(margin, 0))
    passed = jax.random.randint(jax.random.fold_in(own, 4), (amount // 2,), 0, 1 << 20) % (margin + 1)
    tallies = tallies.at[giver].add(-passed).at[sink].add(passed)
    labels = jnp.searchsorted(jnp.cumsum(tallies), jnp.arange(rows * top), side="right").astype(jnp.int32)
    listing = labels.reshape(top, rows).T
    listing = listing[jax.random.permutation(jax.random.fold_in(own, 1), rows)]
    rotation = jax.random.randint(jax.random.fold_in(own, 2), (rows, 1), 0, top)
    return jnp.take_along_axis(listing, (jnp.arange(top)[None, :] + rotation) % top, axis=1)


def portions_of(amount, total, reach, skew, full):
    weights = [(1 << 20) // math.isqrt(rank ** skew) + 1 for rank in range(1, amount + 1)]
    largest = reach if full else min(reach, max(-(-total // amount), total * weights[0] // sum(weights)))
    least = 1 if total - largest >= amount - 1 else 0
    given, spare = [largest] + [least] * (amount - 1), total - largest - least * (amount - 1)
    while spare > 0:
        free = [i for i in range(1, amount) if given[i] < largest] or [i for i in range(1, amount) if given[i] < reach]
        whole, left = sum([weights[i] for i in free]), spare
        for i in free:
            addition = min(reach - given[i], max(1, left * weights[i] // whole), spare)
            given[i] = given[i] + addition
            spare = spare - addition
    return np.array(given)


def bell_draw(rng, dims, scale, limit, pieces=(), held_as=jnp.bfloat16):
    array = scale * jax.random.normal(rng, dims, jnp.float32)
    if pieces:
        array = array * steps_of(rng, dims, pieces, -0.22, 0.18)
    return jnp.clip(array, -limit, limit).astype(held_as)


def setup_inputs(seed: int = 0) -> dict:
    key_list = jax.random.split(jax.random.key(seed), 12)
    tokens = bell_draw(key_list[0], (TOKENS, D), 1.0, 6.0, ((0, 16),))
    norm_gain = jnp.clip(1.0 + 0.18 * jax.random.normal(key_list[1], (D,), jnp.float32), 0.1, 1.9)
    router = bell_draw(key_list[2], (D, EXPERTS), D ** -0.5, 0.125)
    expert_ids_keys = jax.random.split(jax.random.fold_in(key_list[3], 1), TOKENS // TOK_DEV)
    expert_ids_turns = jax.random.permutation(jax.random.fold_in(key_list[3], 3), TOKENS // TOK_DEV)
    expert_ids = jax.vmap(lambda own, number: deal_out(jax.random.fold_in(key_list[3], 2), own, number, TOK_DEV, EXPERTS, TOP, CAP, 1))(expert_ids_keys, expert_ids_turns).reshape((TOKENS, TOP))
    modality = draw_modality(jax.random.fold_in(key_list[11], 71), 0)
    expert_gate = bell_draw(key_list[5], (EXPERTS, D, FF), D ** -0.5, 0.125, ((0, 8), (2, 2)))
    expert_up = bell_draw(key_list[6], (EXPERTS, D, FF), D ** -0.5, 0.125, ((0, 8), (2, 2)))
    expert_down = bell_draw(key_list[7], (EXPERTS, FF, D), FF ** -0.5, 0.15625, ((0, 8), (1, 2)))
    shared_gate = bell_draw(key_list[8], (2, D, SH), D ** -0.5, 0.125, ((2, 4),))
    shared_up = bell_draw(key_list[9], (2, D, SH), D ** -0.5, 0.125, ((2, 4),))
    shared_down = bell_draw(key_list[10], (2, SH, D), SH ** -0.5, 0.21875, ((1, 4),))
    return {"tokens": tokens, "norm_gain": norm_gain, "router": router, "expert_ids": expert_ids, "modality": modality, "expert_gate": expert_gate, "expert_up": expert_up, "expert_down": expert_down, "shared_gate": shared_gate, "shared_up": shared_up, "shared_down": shared_down}


epsilon = 1e-06

def rms_normed(tokens, norm_gain):
    values = tokens.astype(jnp.float32)
    inv_scale = lax.rsqrt(lax.optimization_barrier(jnp.mean(values * values, axis=-1, keepdims=True)) + epsilon)
    return (values * inv_scale * norm_gain).astype(jnp.bfloat16)

def route_weights(normed, router, expert_ids):
    logits = jnp.dot(normed, router, preferred_element_type=jnp.float32)
    chosen = jnp.take_along_axis(logits, expert_ids, axis=1)
    scores = jax.nn.sigmoid(chosen)
    return scores / lax.optimization_barrier(jnp.sum(scores, axis=1, keepdims=True))

def capacity_slots(expert_ids, expert_count, block_rows):
    row_count, top_count = expert_ids.shape
    onehot = (expert_ids[:, :, None] == jnp.arange(expert_count, dtype=jnp.int32)[None, None, :]).astype(jnp.int32)
    grouped = onehot.reshape(row_count // block_rows, block_rows * top_count, expert_count)
    running = (jnp.cumsum(grouped, axis=1, dtype=jnp.int32) - 1).reshape(row_count, top_count, expert_count)
    return lax.optimization_barrier(jnp.sum(running * onehot, axis=-1, dtype=jnp.int32)).astype(jnp.int32)

def reference(tokens, norm_gain, router, expert_ids, modality, expert_gate, expert_up, expert_down, shared_gate, shared_up, shared_down):
    normed = rms_normed(tokens, norm_gain)
    weights = route_weights(normed, router, expert_ids)
    slot_rank = capacity_slots(expert_ids, EXPERTS, TOK_DEV)
    sources = TOKENS // TOK_DEV
    token_index = jnp.broadcast_to(jnp.arange(TOKENS, dtype=jnp.int32)[:, None], (TOKENS, TOP)).astype(jnp.int32)
    source_block = (token_index // TOK_DEV).astype(jnp.int32)
    slot_table = jnp.full((EXPERTS, sources, CAP), TOKENS, jnp.int32)
    slot_table = slot_table.at[expert_ids, source_block, slot_rank].set(token_index)
    weight_table = jnp.zeros((EXPERTS, sources, CAP), jnp.float32)
    weight_table = weight_table.at[expert_ids, source_block, slot_rank].set(weights)
    padded = jnp.concatenate([normed, jnp.zeros((1, D), jnp.bfloat16)], axis=0)

    def one_expert(routed, operands):
        rows_index, slot_weight, gate_weight, up_weight, down_weight = operands
        flat_index = rows_index.reshape(-1)
        gathered = padded[flat_index]
        gate_value = jnp.dot(gathered, gate_weight, preferred_element_type=jnp.float32)
        up_value = jnp.dot(gathered, up_weight, preferred_element_type=jnp.float32)
        hidden = (jax.nn.silu(gate_value) * up_value).astype(jnp.bfloat16)
        result = jnp.dot(hidden, down_weight, preferred_element_type=jnp.float32)
        result = result * slot_weight.reshape(-1)[:, None]
        return (routed.at[flat_index].add(result), None)
    start = jnp.zeros((TOKENS + 1, D), jnp.float32)
    routed, unused = lax.scan(one_expert, start, (slot_table, weight_table, expert_gate, expert_up, expert_down))
    routed = routed[:TOKENS]

    def shared_out(modal_index):
        gate_value = jnp.dot(normed, shared_gate[modal_index], preferred_element_type=jnp.float32)
        up_value = jnp.dot(normed, shared_up[modal_index], preferred_element_type=jnp.float32)
        hidden = (jax.nn.silu(gate_value) * up_value).astype(jnp.bfloat16)
        return jnp.dot(hidden, shared_down[modal_index], preferred_element_type=jnp.float32)
    is_image = (modality == 1)[:, None]
    shared = jnp.where(is_image, shared_out(0), shared_out(1))
    return (shared + routed).astype(jnp.bfloat16)
```

```python
import jax
import jax.numpy as jnp
from jax import lax
from jax.experimental import pallas as pl
from jax.experimental.pallas import tpu as pltpu
from jax.sharding import PartitionSpec as P

epsilon = 1e-06
LANES = 128
MIB = 2**20
NT = (((1,), (1,)), ((), ()))
TN = (((0,), (0,)), ((), ()))


def dot(a, b, dims):
    return lax.dot_general(a, b, dims, preferred_element_type=jnp.float32)


def ring_order(count):
    return list(range(0, count, 2)) + list(range(count - 1, 0, -2))


def call(body, outs, args, name, limit, flops=0, moved=0):
    vmem = pl.BlockSpec(memory_space=pltpu.VMEM)
    return pl.pallas_call(
        body,
        out_shape=outs,
        in_specs=[vmem] * len(args),
        out_specs=jax.tree.map(lambda _: vmem, outs),
        compiler_params=pltpu.CompilerParams(vmem_limit_bytes=limit * MIB),
        cost_estimate=pl.CostEstimate(flops=flops, bytes_accessed=moved, transcendentals=0),
        name=name,
    )(*args)


def prologue_body(expert_count, tokens, gain, router, ids, modality, packed):
    width = tokens.shape[1]
    values = tokens[...].astype(jnp.float32)
    scale = lax.rsqrt(jnp.mean(values * values, axis=1, keepdims=True) + epsilon)
    normed = (values * scale * gain[...]).astype(jnp.bfloat16)
    packed[:, :width] = normed
    scores = 1.0 / (1.0 + jnp.exp(-dot(router[...], normed, NT)))
    which = lax.broadcasted_iota(jnp.int32, scores.shape, 0)
    chosen = which == ids[0:1, :]
    for k in range(1, ids.shape[0]):
        chosen = chosen | (which == ids[k : k + 1, :])
    scores = jnp.where(chosen, scores, 0.0)
    weights = scores / jnp.sum(scores, axis=0, keepdims=True)
    rounded = weights.astype(jnp.bfloat16).astype(jnp.float32)
    image = (modality[...] == 1).astype(jnp.float32)
    rows = packed.shape[1] - width - 2 * expert_count
    first = lax.broadcasted_iota(jnp.int32, (rows, image.shape[1]), 0) == 0
    table = jnp.concatenate([rounded, weights - rounded, jnp.where(first, image, 0.0)], axis=0)
    packed[:, width:] = table.T.astype(jnp.bfloat16)


def side_rows(packed, width, lanes):
    side = packed[:, width:]
    lane = lax.broadcasted_iota(jnp.int32, (8, side.shape[1]), 1)
    picked = lane == lanes[0]
    for other in lanes[1:]:
        picked = picked | (lane == other)
    return dot(picked.astype(jnp.bfloat16), side, NT)[0:1, :]


def gated(gate, up, factor):
    return (gate / (1.0 + jnp.exp(-gate)) * up * factor).astype(jnp.bfloat16)


def expert_body(expert_count, inputs, *refs):
    blocks, (gate, up, down), outs = refs[:inputs], refs[inputs : inputs + 3], refs[inputs + 3 :]
    width = gate.shape[1]
    rows = blocks[0][...]
    if inputs == 2:
        rows = jnp.concatenate([rows, blocks[1][...]], axis=0)
    me = lax.axis_index("expert")
    factor = side_rows(rows, width, (me, me + expert_count))
    rows = rows[:, :width]
    hidden = gated(dot(gate[...], rows, NT), dot(up[...], rows, NT), factor)
    result = dot(hidden, down[...], TN)
    start = 0
    for out in outs:
        out[...] = result[start : start + out.shape[0]].astype(out.dtype)
        start += out.shape[0]


def shared_body(expert_count, own, other, gate, up, down, own_out, other_out):
    width = gate.shape[1]
    rows = jnp.concatenate([own[...], other[...]], axis=0)
    image = side_rows(rows, width, (2 * expert_count,))
    rows = rows[:, :width]
    gate_value, up_value = dot(gate[...], rows, NT), dot(up[...], rows, NT)
    kind = lax.broadcasted_iota(jnp.int32, gate_value.shape, 0) < gate_value.shape[0] // 2
    hidden = gated(gate_value, up_value, jnp.where(kind, image, 1.0 - image))
    result = dot(hidden, down[...], TN)
    own_out[...] = result[: own_out.shape[0]]
    other_out[...] = result[own_out.shape[0] :].astype(other_out.dtype)


def first_add_body(mine, partner, arrived, out):
    total = mine[...] + partner[...].astype(jnp.float32)
    out[...] = total.astype(out.dtype)
    half = arrived.shape[0]
    start = pl.multiple_of((1 - lax.axis_index("tensor")) * half, half)
    place = pl.ds(start, half)
    part = mine[place, :] + partner[place, :].astype(jnp.float32)
    out[place, :] = (part + arrived[...].astype(jnp.float32)).astype(out.dtype)


def last_add_body(*refs):
    terms, (stay, cross) = refs[:-2], refs[-2:]
    half = stay.shape[1]
    core = lax.axis_index("tensor")
    for out, index in ((stay, core), (cross, 1 - core)):
        place = pl.ds(pl.multiple_of(index * half, half), half)
        total = terms[0][:, place].astype(jnp.float32)
        for term in terms[1:]:
            total = total + term[:, place].astype(jnp.float32)
        out[...] = total.astype(out.dtype)


def per_device(
    tokens,
    norm_gain,
    router,
    expert_ids,
    modality,
    expert_gate,
    expert_up,
    expert_down,
    shared_gate,
    shared_up,
    shared_down,
):
    tok_rows, width = tokens.shape
    half_rows, half_width = tok_rows // 2, width // 2
    experts = lax.axis_size("expert")
    side = -(-(2 * experts + 1) // LANES) * LANES
    middle = experts // 2
    shape = jax.ShapeDtypeStruct
    f32, bf16 = jnp.float32, jnp.bfloat16

    order = ring_order(experts)
    onward, across = [], []
    for here, there in zip(order, order[1:] + order[:1]):
        onward += [(2 * here, 2 * there), (2 * there + 1, 2 * here + 1)]
        across += [(2 * here, 2 * there + 1), (2 * there + 1, 2 * here)]
    hop = lambda x: lax.ppermute(x, ("expert", "tensor"), onward)
    cross_hop = lambda x: lax.ppermute(x, ("expert", "tensor"), across)
    swap = lambda x: lax.ppermute(x, "tensor", [(0, 1), (1, 0)])
    dp_swap = lambda x: lax.ppermute(x, "dp", [(0, 1), (1, 0)])

    gate, up = expert_gate[0].T, expert_up[0].T
    down = expert_down[0]
    hidden_units = down.shape[0]
    shared_units = 2 * shared_down.shape[1]
    shared_gate = jnp.swapaxes(shared_gate, 1, 2).reshape(shared_units, width)
    shared_up = jnp.swapaxes(shared_up, 1, 2).reshape(shared_units, width)
    shared_down = shared_down.reshape(shared_units, width)

    own = call(
        lambda *refs: prologue_body(experts, *refs),
        shape((tok_rows, width + side), bf16),
        (tokens, norm_gain[None, :], router.T, expert_ids.T, modality[None, :]),
        "prologue",
        12,
        4 * MIB,
        MIB,
    )

    def experts_of(blocks, outs):
        rows = sum(block.shape[0] for block in blocks)
        return call(
            lambda *refs: expert_body(experts, len(blocks), *refs),
            outs,
            (*blocks, gate, up, down),
            "experts",
            20,
            6 * rows * width * hidden_units,
            6 * width * hidden_units,
        )

    other_dp = dp_swap(own)
    kept, sent = {}, {}
    block = own
    for k in range(1, middle + 1):
        if k == middle:
            start = lax.axis_index("tensor") * half_rows
            block = lax.dynamic_slice_in_dim(block, start, half_rows, axis=0)
        block = hop(block)
        partner = swap(block)
        rows = block.shape[0]
        give, kept[k] = experts_of(
            (block, partner), (shape((rows, width), bf16), shape((rows, width), f32))
        )
        sent[k] = swap(give)

    own_part = experts_of((own,), (shape((tok_rows, width), f32),))[0]
    shared_own, shared_other = call(
        lambda *refs: shared_body(experts, *refs),
        (shape((tok_rows, width), f32), shape((tok_rows, width), bf16)),
        (own, other_dp, shared_gate, shared_up, shared_down),
        "shared",
        16,
        12 * tok_rows * width * shared_units,
        6 * width * shared_units,
    )
    shared_back = dp_swap(shared_other)
    halves = (shape((tok_rows, half_width), bf16),) * 2
    local_stay, local_cross = call(
        last_add_body, (shape((tok_rows, half_width), f32), halves[0]),
        (own_part, shared_own, shared_back), "local_add", 8,
    )
    local_recv = swap(local_cross)

    running = (kept[middle] + sent[middle].astype(f32)).astype(bf16)
    for k in range(middle - 1, 0, -1):
        arrived = hop(running)
        if k == 1:
            stay, cross = call(
                last_add_body, halves, (kept[k], sent[k], arrived), "last_add", 8
            )
        elif k == middle - 1:
            running = call(
                first_add_body, shape((tok_rows, width), bf16),
                (kept[k], sent[k], arrived), "first_add", 8,
            )
        else:
            running = (kept[k] + sent[k].astype(f32) + arrived.astype(f32)).astype(bf16)
    stay, cross = hop(stay), cross_hop(cross)
    total = local_stay + local_recv.astype(f32) + stay.astype(f32) + cross.astype(f32)
    return total.astype(bf16)


def solution(mesh):
    in_specs = (
        P(("dp", "expert"), None),
        P(),
        P(),
        P(("dp", "expert"), None),
        P(("dp", "expert")),
        P("expert", None, "tensor"),
        P("expert", None, "tensor"),
        P("expert", "tensor", None),
        P(None, None, ("dp", "tensor")),
        P(None, None, ("dp", "tensor")),
        P(None, ("dp", "tensor"), None),
    )
    out_specs = P(("dp", "expert"), "tensor")
    return jax.shard_map(
        per_device, mesh=mesh, in_specs=in_specs, out_specs=out_specs, check_vma=False
    )
```

```python
import jax
import jax.numpy as jnp
from jax import lax
from jax.experimental import pallas as pl
from jax.experimental.pallas import tpu as pltpu
from jax.sharding import PartitionSpec as P


epsilon = 1e-06
LANES = 128
MIB = 2**20
NT = (((1,), (1,)), ((), ()))
TN = (((0,), (0,)), ((), ()))


def dot(a, b, dims):
    return lax.dot_general(a, b, dims, preferred_element_type=jnp.float32)


def ring_order(count):
    return list(range(0, count, 2)) + list(range(count - 1, 0, -2))


def call(body, outs, args, limit, flops=0, moved=0, scratch=()):
    vmem = pl.BlockSpec(memory_space=pltpu.VMEM)
    return pl.pallas_call(
        body,
        out_shape=outs,
        in_specs=[vmem] * len(args),
        out_specs=jax.tree.map(lambda _: vmem, outs),
        scratch_shapes=scratch,
        compiler_params=pltpu.CompilerParams(vmem_limit_bytes=limit * MIB),
        cost_estimate=pl.CostEstimate(flops=flops, bytes_accessed=moved, transcendentals=0),
    )(*args)


def lead_body(out):
    out[...] = jnp.zeros_like(out)


def prologue_body(expert_count, lead, tokens, gain, router, ids, modality, packed, part):
    width = tokens.shape[1]
    values = tokens[...].astype(jnp.float32)
    scale = lax.rsqrt(jnp.mean(values * values, axis=1, keepdims=True) + epsilon)
    normed = (values * scale * gain[...]).astype(jnp.bfloat16)
    packed[:, :width] = normed
    scores = 1.0 / (1.0 + jnp.exp(-dot(router[...], normed, NT)))
    which = lax.broadcasted_iota(jnp.int32, scores.shape, 0)
    chosen = which == ids[0:1, :]
    for k in range(1, ids.shape[0]):
        chosen = chosen | (which == ids[k : k + 1, :])
    scores = jnp.where(chosen, scores, 0.0)
    weights = scores / jnp.sum(scores, axis=0, keepdims=True)
    rounded = weights.astype(jnp.bfloat16).astype(jnp.float32)
    image = (modality[...] == 1).astype(jnp.float32)
    rows = packed.shape[1] - width - 2 * expert_count
    first = lax.broadcasted_iota(jnp.int32, (rows, image.shape[1]), 0) == 0
    table = jnp.concatenate([rounded, weights - rounded, jnp.where(first, image, 0.0)], axis=0)
    packed[:, width:] = table.T.astype(jnp.bfloat16)
    half = part.shape[0]
    start = pl.multiple_of(lax.axis_index("tensor") * half, half)
    part[...] = packed[pl.ds(start, half), :]


def side_rows(rows, width, lanes):
    side = rows[:, width:]
    lane = lax.broadcasted_iota(jnp.int32, (8, side.shape[1]), 1)
    picked = lane == lanes[0]
    for other in lanes[1:]:
        picked = picked | (lane == other)
    return dot(picked.astype(jnp.bfloat16), side, NT)[0:1, :]


def gated(gate, up, factor):
    return (gate / (1.0 + jnp.exp(-gate)) * up * factor).astype(jnp.bfloat16)


def expert_hidden(expert_count, rows, gate, up):
    width = gate.shape[1]
    me = lax.axis_index("expert")
    factor = side_rows(rows, width, (me, me + expert_count))
    rows = rows[:, :width]
    return gated(dot(gate[...], rows, NT), dot(up[...], rows, NT), factor)


def pair_body(expert_count, up_own, down_own, up_other, down_other, gate, up, down, keep, give, rows):
    half = up_own.shape[0]
    mine = pl.multiple_of(lax.axis_index("tensor") * half, half)
    theirs = pl.multiple_of((1 - lax.axis_index("tensor")) * half, half)
    for base, own, other in ((0, up_own, up_other), (2 * half, down_own, down_other)):
        rows[pl.ds(base + mine, half), :] = own[...]
        rows[pl.ds(base + theirs, half), :] = other[...]
    split_down(expert_hidden(expert_count, rows[...], gate, up), down, keep, give)


def column_halves(hidden, down):
    half = down.shape[1] // 2
    core = lax.axis_index("tensor")
    places = [pl.ds(pl.multiple_of(i * half, half), half) for i in (core, 1 - core)]
    return [dot(hidden, down[:, place], TN) for place in places]


def split_down(hidden, down, keep, give):
    mine, theirs = column_halves(hidden, down)
    keep[...] = mine
    give[...] = theirs.astype(give.dtype)


def own_body(expert_count, own, gate, up, down, mine, theirs):
    hidden = expert_hidden(expert_count, own[...], gate, up)
    mine[...], theirs[...] = column_halves(hidden, down)


def far_body(expert_count, up_own, down_own, up_other, down_other, gate, up, down, keep, give, rows):
    part = up_own.shape[0]
    mine = pl.multiple_of(lax.axis_index("tensor") * 2 * part, 2 * part)
    theirs = pl.multiple_of((1 - lax.axis_index("tensor")) * 2 * part, 2 * part)
    rows[pl.ds(mine, part), :] = up_own[...]
    rows[pl.ds(mine + part, part), :] = down_own[...]
    rows[pl.ds(theirs, part), :] = up_other[...]
    rows[pl.ds(theirs + part, part), :] = down_other[...]
    split_down(expert_hidden(expert_count, rows[...], gate, up), down, keep, give)


def shared_body(expert_count, own, other, mine, theirs, gate, up, down, keep, give):
    width = gate.shape[1]
    rows = jnp.concatenate([own[...], other[...]], axis=0)
    image = side_rows(rows, width, (2 * expert_count,))
    rows = rows[:, :width]
    gate_value, up_value = dot(gate[...], rows, NT), dot(up[...], rows, NT)
    kind = lax.broadcasted_iota(jnp.int32, gate_value.shape, 0) < gate_value.shape[0] // 2
    hidden = gated(gate_value, up_value, jnp.where(kind, image, 1.0 - image))
    count = own.shape[0]
    for out, result, first in zip((keep, give), column_halves(hidden, down), (mine, theirs)):
        out[:count, :] = (result[:count] + first[...]).astype(out.dtype)
        out[count:, :] = result[count:].astype(out.dtype)


def far_add_body(keep, recv, upward, downward):
    half = upward.shape[0]
    total = keep[...] + recv[...].astype(jnp.float32)
    upward[...] = total[:half].astype(upward.dtype)
    downward[...] = total[half:].astype(downward.dtype)


def sum_body(bases, keep, recv, *refs):
    outs = refs[-len(bases) :]
    for index, (base, out) in enumerate(zip(bases, outs)):
        place = slice(base, base + out.shape[0])
        total = keep[place, :] + recv[place, :].astype(jnp.float32)
        if len(refs) > len(outs):
            total = total + refs[index][...].astype(jnp.float32)
        out[...] = total.astype(out.dtype)


def total_body(local, other, ahead_one, ahead_two, back_one, back_two, out):
    half = ahead_one.shape[0]
    for index, (one, two) in enumerate(((ahead_one, back_one), (ahead_two, back_two))):
        place = slice(index * half, index * half + half)
        total = local[place, :] + other[place, :].astype(jnp.float32)
        total = total + one[...].astype(jnp.float32) + two[...].astype(jnp.float32)
        out[place, :] = total.astype(out.dtype)


def per_device(
    tokens,
    norm_gain,
    router,
    expert_ids,
    modality,
    expert_gate,
    expert_up,
    expert_down,
    shared_gate,
    shared_up,
    shared_down,
):
    count, width = tokens.shape
    half, columns = count // 2, width // 2
    quarter = half // 2
    experts = lax.axis_size("expert")
    side = -(-(2 * experts + 1) // LANES) * LANES
    middle = experts // 2
    shape = jax.ShapeDtypeStruct
    f32, bf16 = jnp.float32, jnp.bfloat16

    order = ring_order(experts)
    onward = list(zip(order, order[1:] + order[:1]))
    backward = [(b, a) for a, b in onward]
    ahead = lambda x: lax.ppermute(x, "expert", onward)
    back = lambda x: lax.ppermute(x, "expert", backward)
    swap = lambda x: lax.ppermute(x, "tensor", [(0, 1), (1, 0)])
    dp_swap = lambda x: lax.ppermute(x, "dp", [(0, 1), (1, 0)])

    hidden_units = expert_down.shape[1]
    shared_units = 2 * shared_down.shape[1]
    stored = (
        expert_gate[0].T,
        expert_up[0].T,
        expert_down[0],
        jnp.swapaxes(shared_gate, 1, 2).reshape(shared_units, width),
        jnp.swapaxes(shared_up, 1, 2).reshape(shared_units, width),
        shared_down.reshape(shared_units, width),
    )
    inputs = (tokens, norm_gain[None, :], router.T, expert_ids.T, modality[None, :])
    lead = call(lead_body, shape((8, LANES), f32), (), 1, 2**34, MIB)
    own, part = call(
        lambda *refs: prologue_body(experts, *refs),
        (shape((count, width + side), bf16), shape((half, width + side), bf16)),
        (lead, *inputs),
        8,
        4 * MIB,
        MIB,
    )
    other = dp_swap(own)
    up_block, down_block = ahead(part), back(part)
    weights = stored

    def experts_of(body, *blocks):
        rows = 4 * blocks[0].shape[0]
        return call(
            lambda *refs: body(experts, *refs),
            (shape((rows, columns), f32), shape((rows, columns), bf16)),
            (*blocks, *weights[:3]),
            16,
            6 * rows * width * hidden_units,
            6 * width * hidden_units,
            [pltpu.VMEM((rows, width + side), bf16)],
        )

    def own_part(own):
        return call(
            lambda *refs: own_body(experts, *refs),
            (shape((count, columns), f32),) * 2,
            (own, *weights[:3]),
            16,
            6 * count * width * hidden_units,
            6 * width * hidden_units,
        )

    def shared_part(*values):
        return call(
            lambda *refs: shared_body(experts, *refs),
            (shape((2 * count, columns), f32), shape((2 * count, columns), bf16)),
            (*values, *weights[3:]),
            16,
            12 * shared_units * count * width,
            6 * width * shared_units,
        )

    def sums(k, bases, *arrived):
        return call(
            lambda *refs: sum_body(bases, *refs),
            (shape((half, columns), bf16),) * len(bases),
            (keep[k], recv[k], *arrived),
            8,
        )

    keep, recv = {}, {}
    own_sums = own_part(own)
    for k in range(1, middle + 1):
        rows = [up_block, down_block]
        if k == middle - 1:
            up_block, down_block = up_block[:quarter], down_block[quarter:]
        if k < middle:
            up_block = ahead(up_block)
            down_block = back(down_block)
        rows += [swap(rows[0]), swap(rows[1])]
        keep[k], give = experts_of(pair_body if k < middle else far_body, *rows)
        recv[k] = swap(give)

    ahead_base, back_base = count, 0
    short = sums(middle - 1, (ahead_base + half, back_base))
    long = call(far_add_body, (shape((half, columns), bf16),) * 2, (keep[middle], recv[middle]), 8)

    def travel(pair):
        return ahead(pair[0]), back(pair[1])

    for k in range(middle - 1, 0, -1):
        short = travel(short)
        long = travel(long)
        if k > 1:
            for way, base in enumerate((ahead_base + half, back_base)):
                part = sums(k - 1, (base,), short[way])
                short = (*part, short[1]) if way == 0 else (short[0], *part)
        for way, base in enumerate((ahead_base, back_base + half)):
            part = sums(k, (base,), long[way])
            long = (*part, long[1]) if way == 0 else (long[0], *part)
    long = travel(long)

    local, give = shared_part(own, other, *own_sums)
    local = local + swap(give).astype(f32)
    local_other = dp_swap(local[count:].astype(bf16))
    return call(
        total_body,
        shape((count, columns), bf16),
        (local, local_other, long[0], short[0], short[1], long[1]),
        8,
    )


def solution(mesh):
    in_specs = (
        P(("dp", "expert"), None),
        P(),
        P(),
        P(("dp", "expert"), None),
        P(("dp", "expert")),
        P("expert", None, "tensor"),
        P("expert", None, "tensor"),
        P("expert", "tensor", None),
        P(None, None, ("dp", "tensor")),
        P(None, None, ("dp", "tensor")),
        P(None, ("dp", "tensor"), None),
    )
    out_specs = P(("dp", "expert"), "tensor")

    return jax.shard_map(
        per_device, mesh=mesh, in_specs=in_specs, out_specs=out_specs, check_vma=False
    )
```

```python
import jax
import jax.numpy as jnp
from jax import lax
from jax.experimental import pallas as pl
from jax.experimental.pallas import tpu as pltpu
from jax.sharding import PartitionSpec as P


epsilon = 1e-06
LANES = 128
MIB = 2**20
NT = (((1,), (1,)), ((), ()))
TN = (((0,), (0,)), ((), ()))


def dot(a, b, dims):
    return lax.dot_general(a, b, dims, preferred_element_type=jnp.float32)


def ring_order(count):
    return list(range(0, count, 2)) + list(range(count - 1, 0, -2))


def call(body, outs, args, limit, flops=0, moved=0, scratch=()):
    vmem = pl.BlockSpec(memory_space=pltpu.VMEM)
    return pl.pallas_call(
        body,
        out_shape=outs,
        in_specs=[vmem] * len(args),
        out_specs=jax.tree.map(lambda _: vmem, outs),
        scratch_shapes=scratch,
        compiler_params=pltpu.CompilerParams(vmem_limit_bytes=limit * MIB),
        cost_estimate=pl.CostEstimate(flops=flops, bytes_accessed=moved, transcendentals=0),
    )(*args)


def lead_body(out):
    out[...] = jnp.zeros_like(out)


def prologue_body(expert_count, lead, tokens, gain, router, ids, modality, packed, lower, upper):
    width = tokens.shape[1]
    values = tokens[...].astype(jnp.float32)
    scale = lax.rsqrt(jnp.mean(values * values, axis=1, keepdims=True) + epsilon)
    normed = (values * scale * gain[...]).astype(jnp.bfloat16)
    packed[:, :width] = normed
    scores = 1.0 / (1.0 + jnp.exp(-dot(router[...], normed, NT)))
    which = lax.broadcasted_iota(jnp.int32, scores.shape, 0)
    chosen = which == ids[0:1, :]
    for k in range(1, ids.shape[0]):
        chosen = chosen | (which == ids[k : k + 1, :])
    scores = jnp.where(chosen, scores, 0.0)
    weights = scores / jnp.sum(scores, axis=0, keepdims=True)
    rounded = weights.astype(jnp.bfloat16).astype(jnp.float32)
    image = (modality[...] == 1).astype(jnp.float32)
    rows = packed.shape[1] - width - 2 * expert_count
    first = lax.broadcasted_iota(jnp.int32, (rows, image.shape[1]), 0) == 0
    table = jnp.concatenate([rounded, weights - rounded, jnp.where(first, image, 0.0)], axis=0)
    packed[:, width:] = table.T.astype(jnp.bfloat16)
    part = lower.shape[0]
    start = pl.multiple_of(lax.axis_index("tensor") * 2 * part, 2 * part)
    lower[...] = packed[pl.ds(start, part), :]
    upper[...] = packed[pl.ds(start + part, part), :]


def side_rows(rows, width, lanes):
    side = rows[:, width:]
    lane = lax.broadcasted_iota(jnp.int32, (8, side.shape[1]), 1)
    picked = lane == lanes[0]
    for other in lanes[1:]:
        picked = picked | (lane == other)
    return dot(picked.astype(jnp.bfloat16), side, NT)[0:1, :]


def gated(gate, up, factor):
    return (gate / (1.0 + jnp.exp(-gate)) * up * factor).astype(jnp.bfloat16)


def expert_hidden(expert_count, rows, gate, up):
    width = gate.shape[1]
    me = lax.axis_index("expert")
    factor = side_rows(rows, width, (me, me + expert_count))
    rows = rows[:, :width]
    return gated(dot(gate[...], rows, NT), dot(up[...], rows, NT), factor)


def pack_body(*refs):
    part = refs[0].shape[0]
    for index, piece in enumerate(refs[:-1]):
        refs[-1][index * part : (index + 1) * part, :] = piece[...]


def pair_body(expert_count, mine, theirs, gate, up, down, keep, give, rows):
    half = mine.shape[0] // 2
    core = lax.axis_index("tensor")
    for index, pieces in ((core, mine), (1 - core, theirs)):
        for block in range(2):
            start = pl.multiple_of((2 * block + index) * half, half)
            rows[pl.ds(start, half), :] = pieces[block * half : (block + 1) * half, :]
    split_down(expert_hidden(expert_count, rows[...], gate, up), down, keep, give)


def column_place(down, whose):
    half = down.shape[1] // 2
    core = lax.axis_index("tensor")
    return pl.ds(pl.multiple_of((1 - core if whose else core) * half, half), half)


def column_halves(hidden, down):
    return [dot(hidden, down[:, column_place(down, whose)], TN) for whose in range(2)]


def split_down(hidden, down, keep, give):
    mine, theirs = column_halves(hidden, down)
    keep[...] = mine
    give[...] = theirs.astype(give.dtype)


def own_body(expert_count, own, gate, up, down, mine, theirs):
    hidden = expert_hidden(expert_count, own[...], gate, up)
    mine[...], theirs[...] = column_halves(hidden, down)


def far_body(expert_count, mine, theirs, gate, up, down, give, hidden, rows):
    half = mine.shape[0]
    core = lax.axis_index("tensor")
    for index, piece in ((core, mine), (1 - core, theirs)):
        rows[pl.ds(pl.multiple_of(index * half, half), half), :] = piece[...]
    hidden[...] = expert_hidden(expert_count, rows[...], gate, up)
    give[...] = dot(hidden[...], down[:, column_place(down, 1)], TN).astype(give.dtype)


def far_keep_body(hidden, down, keep):
    keep[...] = dot(hidden[...], down[:, column_place(down, 0)], TN)


def shared_body(expert_count, own, other, mine, theirs, gate, up, down, keep, give):
    width = gate.shape[1]
    rows = jnp.concatenate([own[...], other[...]], axis=0)
    image = side_rows(rows, width, (2 * expert_count,))
    rows = rows[:, :width]
    gate_value, up_value = dot(gate[...], rows, NT), dot(up[...], rows, NT)
    kind = lax.broadcasted_iota(jnp.int32, gate_value.shape, 0) < gate_value.shape[0] // 2
    hidden = gated(gate_value, up_value, jnp.where(kind, image, 1.0 - image))
    count = own.shape[0]
    for out, result, first in zip((keep, give), column_halves(hidden, down), (mine, theirs)):
        out[:count, :] = (result[:count] + first[...]).astype(out.dtype)
        out[count:, :] = result[count:].astype(out.dtype)


def far_add_body(keep, recv, upward, downward):
    half = upward.shape[0]
    total = keep[...] + recv[...].astype(jnp.float32)
    upward[...] = total[:half].astype(upward.dtype)
    downward[...] = total[half:].astype(downward.dtype)


def sum_body(bases, keep, recv, *refs):
    outs = refs[-len(bases) :]
    for index, (base, out) in enumerate(zip(bases, outs)):
        place = slice(base, base + out.shape[0])
        total = keep[place, :] + recv[place, :].astype(jnp.float32)
        if len(refs) > len(outs):
            total = total + refs[index][...].astype(jnp.float32)
        out[...] = total.astype(out.dtype)


def total_body(local, other, ahead_one, ahead_two, back_one, back_two, out):
    half = ahead_one.shape[0]
    for index, (one, two) in enumerate(((ahead_one, back_one), (ahead_two, back_two))):
        place = slice(index * half, index * half + half)
        total = local[place, :] + other[place, :].astype(jnp.float32)
        total = total + one[...].astype(jnp.float32) + two[...].astype(jnp.float32)
        out[place, :] = total.astype(out.dtype)


def per_device(
    tokens,
    norm_gain,
    router,
    expert_ids,
    modality,
    expert_gate,
    expert_up,
    expert_down,
    shared_gate,
    shared_up,
    shared_down,
):
    count, width = tokens.shape
    half, columns = count // 2, width // 2
    quarter = half // 2
    experts = lax.axis_size("expert")
    side = -(-(2 * experts + 1) // LANES) * LANES
    middle = experts // 2
    shape = jax.ShapeDtypeStruct
    f32, bf16 = jnp.float32, jnp.bfloat16

    order = ring_order(experts)
    onward = list(zip(order, order[1:] + order[:1]))
    backward = [(b, a) for a, b in onward]
    ahead = lambda x: lax.ppermute(x, "expert", onward)
    back = lambda x: lax.ppermute(x, "expert", backward)
    swap = lambda x: lax.ppermute(x, "tensor", [(0, 1), (1, 0)])
    dp_swap = lambda x: lax.ppermute(x, "dp", [(0, 1), (1, 0)])

    hidden_units = expert_down.shape[1]
    shared_units = 2 * shared_down.shape[1]
    stored = (
        expert_gate[0].T,
        expert_up[0].T,
        expert_down[0],
        jnp.swapaxes(shared_gate, 1, 2).reshape(shared_units, width),
        jnp.swapaxes(shared_up, 1, 2).reshape(shared_units, width),
        shared_down.reshape(shared_units, width),
    )
    inputs = (tokens, norm_gain[None, :], router.T, expert_ids.T, modality[None, :])
    lead = call(lead_body, shape((8, LANES), f32), (), 1, 2**34, MIB)
    own, lower, upper = call(
        lambda *refs: prologue_body(experts, *refs),
        (shape((count, width + side), bf16),) + (shape((quarter, width + side), bf16),) * 2,
        (lead, *inputs),
        8,
        4 * MIB,
        MIB,
    )
    other = dp_swap(own)
    weights = stored

    def pair_part(mine, theirs):
        rows = 2 * mine.shape[0]
        return call(
            lambda *refs: pair_body(experts, *refs),
            (shape((rows, columns), f32), shape((rows, columns), bf16)),
            (mine, theirs, *weights[:3]),
            16,
            6 * rows * width * hidden_units,
            6 * width * hidden_units,
            [pltpu.VMEM((rows, width + side), bf16)],
        )

    def far_part(mine, theirs):
        return call(
            lambda *refs: far_body(experts, *refs),
            (shape((count, columns), bf16), shape((hidden_units, count), bf16)),
            (mine, theirs, *weights[:3]),
            16,
            5 * count * width * hidden_units,
            6 * width * hidden_units,
            [pltpu.VMEM((count, width + side), bf16)],
        )

    def far_keep(hidden):
        return call(
            far_keep_body,
            shape((count, columns), f32),
            (hidden, weights[2]),
            16,
            count * width * hidden_units,
            width * hidden_units,
        )

    def own_part(own):
        return call(
            lambda *refs: own_body(experts, *refs),
            (shape((count, columns), f32),) * 2,
            (own, *weights[:3]),
            16,
            6 * count * width * hidden_units,
            6 * width * hidden_units,
        )

    def shared_part(*values):
        return call(
            lambda *refs: shared_body(experts, *refs),
            (shape((2 * count, columns), f32), shape((2 * count, columns), bf16)),
            (*values, *weights[3:]),
            16,
            12 * shared_units * count * width,
            6 * width * shared_units,
        )

    def sums(k, bases, *arrived):
        return call(
            lambda *refs: sum_body(bases, *refs),
            (shape((half, columns), bf16),) * len(bases),
            (keep[k], recv[k], *arrived),
            8,
        )

    def travel(pair):
        return ahead(pair[0]), back(pair[1])

    def packed(pieces):
        rows = len(pieces) * pieces[0].shape[0]
        return call(pack_body, shape((rows, width + side), bf16), pieces, 4)

    keep, recv = {}, {}
    own_sums = own_part(own)
    long, short = (lower, upper), (upper, lower)
    for k in range(1, middle + 1):
        long = travel(long)
        if k < middle:
            short = travel(short)
            mine = packed((long[0], short[0], short[1], long[1]))
            keep[k], give = pair_part(mine, swap(mine))
        else:
            mine = packed(long)
            give, hidden = far_part(mine, swap(mine))
            keep[k] = far_keep(hidden)
        recv[k] = swap(give)

    ahead_base, back_base = count, 0
    short = sums(middle - 1, (ahead_base + half, back_base))
    long = call(
        far_add_body,
        (shape((half, columns), bf16),) * 2,
        (keep[middle], recv[middle]),
        8,
    )

    for k in range(middle - 1, 0, -1):
        long = travel(long)
        short = travel(short)
        if k > 1:
            for way, base in enumerate((ahead_base + half, back_base)):
                part = sums(k - 1, (base,), short[way])
                short = (*part, short[1]) if way == 0 else (short[0], *part)
        for way, base in enumerate((ahead_base, back_base + half)):
            part = sums(k, (base,), long[way])
            long = (*part, long[1]) if way == 0 else (long[0], *part)
    long = travel(long)

    local, give = shared_part(own, other, *own_sums)
    local = local + swap(give).astype(f32)
    local_other = dp_swap(local[count:].astype(bf16))
    return call(
        total_body,
        shape((count, columns), bf16),
        (local, local_other, long[0], short[0], short[1], long[1]),
        8,
    )


def solution(mesh):
    in_specs = (
        P(("dp", "expert"), None),
        P(),
        P(),
        P(("dp", "expert"), None),
        P(("dp", "expert")),
        P("expert", None, "tensor"),
        P("expert", None, "tensor"),
        P("expert", "tensor", None),
        P(None, None, ("dp", "tensor")),
        P(None, None, ("dp", "tensor")),
        P(None, ("dp", "tensor"), None),
    )
    out_specs = P(("dp", "expert"), "tensor")

    return jax.shard_map(
        per_device, mesh=mesh, in_specs=in_specs, out_specs=out_specs, check_vma=False
    )
```

```python
import jax
import jax.numpy as jnp
from jax import lax
from jax.experimental import pallas as pl
from jax.experimental.pallas import tpu as pltpu
from jax.sharding import PartitionSpec as P


epsilon = 1e-06
LANES = 128
MIB = 2**20
NT = (((1,), (1,)), ((), ()))
TN = (((0,), (0,)), ((), ()))


def dot(a, b, dims):
    return lax.dot_general(a, b, dims, preferred_element_type=jnp.float32)


def ring_order(count):
    return list(range(0, count, 2)) + list(range(count - 1, 0, -2))


def call(body, outs, args, limit, flops=0, moved=0, scratch=()):
    vmem = pl.BlockSpec(memory_space=pltpu.VMEM)
    return pl.pallas_call(
        body,
        out_shape=outs,
        in_specs=[vmem] * len(args),
        out_specs=jax.tree.map(lambda _: vmem, outs),
        scratch_shapes=scratch,
        compiler_params=pltpu.CompilerParams(vmem_limit_bytes=limit * MIB),
        cost_estimate=pl.CostEstimate(flops=flops, bytes_accessed=moved, transcendentals=0),
    )(*args)


def lead_body(out):
    out[...] = jnp.zeros_like(out)


def prologue_body(expert_count, lead, tokens, gain, router, ids, modality, packed, *parts):
    width = tokens.shape[1]
    values = tokens[...].astype(jnp.float32)
    scale = lax.rsqrt(jnp.mean(values * values, axis=1, keepdims=True) + epsilon)
    normed = (values * scale * gain[...]).astype(jnp.bfloat16)
    packed[:, :width] = normed
    scores = 1.0 / (1.0 + jnp.exp(-dot(router[...], normed, NT)))
    which = lax.broadcasted_iota(jnp.int32, scores.shape, 0)
    chosen = which == ids[0:1, :]
    for k in range(1, ids.shape[0]):
        chosen = chosen | (which == ids[k : k + 1, :])
    scores = jnp.where(chosen, scores, 0.0)
    weights = scores / jnp.sum(scores, axis=0, keepdims=True)
    rounded = weights.astype(jnp.bfloat16).astype(jnp.float32)
    image = (modality[...] == 1).astype(jnp.float32)
    count = image.shape[1]
    group = (packed.shape[1] - width) // 2
    rows = group - 2 * expert_count
    first = lax.broadcasted_iota(jnp.int32, (rows, count), 0) == 0
    table = jnp.concatenate([rounded, weights - rounded, jnp.where(first, image, 0.0)], axis=0)
    up_long, down_long, up_short, down_short, both = parts
    part = up_long.shape[0]
    start = pl.multiple_of(lax.axis_index("tensor") * 2 * part, 2 * part)
    places = (pl.ds(start, part), pl.ds(start + part, part))
    for out, place, shift in ((up_long, places[0], count - part), (down_long, places[1], part)):
        pair = jnp.concatenate([table, pltpu.roll(table, shift, 1)], axis=0)
        both[...] = pair.T
        out[:, :width] = packed[place, :width]
        out[:, width:] = both[place, :].astype(jnp.bfloat16)
    up_short[...] = packed[places[1], :width]
    down_short[...] = packed[places[0], :width]
    packed[:, width:] = jnp.concatenate([table, jnp.zeros_like(table)], axis=0).T.astype(jnp.bfloat16)


def side_rows(rows, width, lanes):
    side = rows[:, width:]
    lane = lax.broadcasted_iota(jnp.int32, (8, side.shape[1]), 1)
    picked = lane == lanes[0]
    for other in lanes[1:]:
        picked = picked | (lane == other)
    return dot(picked.astype(jnp.bfloat16), side, NT)[0:1, :]


def gated(gate, up, factor):
    return (gate / (1.0 + jnp.exp(-gate)) * up * factor).astype(jnp.bfloat16)


def expert_hidden(expert_count, rows, gate, up):
    width = gate.shape[1]
    me = lax.axis_index("expert")
    group = (rows.shape[1] - width) // 2
    lanes = [me + base + group * i for base in (0, expert_count) for i in range(2)]
    factor = side_rows(rows, width, lanes)
    rows = rows[:, :width]
    return gated(dot(gate[...], rows, NT), dot(up[...], rows, NT), factor)


def pack_body(width, *refs):
    pieces, out = refs[:-1], refs[-1]
    part = pieces[0].shape[0]
    long = (pieces[0], pieces[-1])
    lane = lax.broadcasted_iota(jnp.int32, (part, out.shape[1] - width), 1)
    led = lane >= lane.shape[1] // 2
    for index, piece in enumerate(pieces):
        place = slice(index * part, (index + 1) * part)
        side = long[2 * index // len(pieces)][:, width:].astype(jnp.float32)
        brought = piece.shape[1] == width
        side = jnp.where(led if brought else jnp.logical_not(led), side, 0.0)
        out[place, :width] = piece[:, :width]
        out[place, width:] = side.astype(out.dtype)


def pair_body(expert_count, mine, theirs, gate, up, down, keep, give, rows):
    half = mine.shape[0] // 2
    core = lax.axis_index("tensor")
    for index, pieces in ((core, mine), (1 - core, theirs)):
        for block in range(2):
            start = pl.multiple_of((2 * block + index) * half, half)
            rows[pl.ds(start, half), :] = pieces[block * half : (block + 1) * half, :]
    split_down(expert_hidden(expert_count, rows[...], gate, up), down, keep, give)


def column_place(down, whose):
    half = down.shape[1] // 2
    core = lax.axis_index("tensor")
    return pl.ds(pl.multiple_of((1 - core if whose else core) * half, half), half)


def column_halves(hidden, down):
    return [dot(hidden, down[:, column_place(down, whose)], TN) for whose in range(2)]


def split_down(hidden, down, keep, give):
    mine, theirs = column_halves(hidden, down)
    keep[...] = mine
    give[...] = theirs.astype(give.dtype)


def own_body(expert_count, own, gate, up, down, mine, theirs):
    hidden = expert_hidden(expert_count, own[...], gate, up)
    mine[...], theirs[...] = column_halves(hidden, down)


def far_body(expert_count, mine, theirs, gate, up, down, give, hidden, rows):
    half = mine.shape[0]
    core = lax.axis_index("tensor")
    for index, piece in ((core, mine), (1 - core, theirs)):
        rows[pl.ds(pl.multiple_of(index * half, half), half), :] = piece[...]
    hidden[...] = expert_hidden(expert_count, rows[...], gate, up)
    give[...] = dot(hidden[...], down[:, column_place(down, 1)], TN).astype(give.dtype)


def far_keep_body(hidden, down, keep):
    keep[...] = dot(hidden[...], down[:, column_place(down, 0)], TN)


def shared_body(expert_count, own, other, mine, theirs, gate, up, down, keep, give):
    width = gate.shape[1]
    rows = jnp.concatenate([own[...], other[...]], axis=0)
    image = side_rows(rows, width, (2 * expert_count,))
    rows = rows[:, :width]
    gate_value, up_value = dot(gate[...], rows, NT), dot(up[...], rows, NT)
    kind = lax.broadcasted_iota(jnp.int32, gate_value.shape, 0) < gate_value.shape[0] // 2
    hidden = gated(gate_value, up_value, jnp.where(kind, image, 1.0 - image))
    count = own.shape[0]
    for out, result, first in zip((keep, give), column_halves(hidden, down), (mine, theirs)):
        out[:count, :] = (result[:count] + first[...]).astype(out.dtype)
        out[count:, :] = result[count:].astype(out.dtype)


def far_add_body(keep, recv, upward, downward):
    half = upward.shape[0]
    total = keep[...] + recv[...].astype(jnp.float32)
    upward[...] = total[:half].astype(upward.dtype)
    downward[...] = total[half:].astype(downward.dtype)


def sum_body(bases, keep, recv, *refs):
    outs = refs[-len(bases) :]
    for index, (base, out) in enumerate(zip(bases, outs)):
        place = slice(base, base + out.shape[0])
        total = keep[place, :] + recv[place, :].astype(jnp.float32)
        if len(refs) > len(outs):
            total = total + refs[index][...].astype(jnp.float32)
        out[...] = total.astype(out.dtype)


def total_body(local, other, ahead_one, ahead_two, back_one, back_two, out):
    half = ahead_one.shape[0]
    for index, (one, two) in enumerate(((ahead_one, back_one), (ahead_two, back_two))):
        place = slice(index * half, index * half + half)
        total = local[place, :] + other[place, :].astype(jnp.float32)
        total = total + one[...].astype(jnp.float32) + two[...].astype(jnp.float32)
        out[place, :] = total.astype(out.dtype)


def per_device(
    tokens,
    norm_gain,
    router,
    expert_ids,
    modality,
    expert_gate,
    expert_up,
    expert_down,
    shared_gate,
    shared_up,
    shared_down,
):
    count, width = tokens.shape
    half, columns = count // 2, width // 2
    quarter = half // 2
    experts = lax.axis_size("expert")
    side = -(-2 * (2 * experts + 1) // LANES) * LANES
    middle = experts // 2
    shape = jax.ShapeDtypeStruct
    f32, bf16 = jnp.float32, jnp.bfloat16

    order = ring_order(experts)
    onward = list(zip(order, order[1:] + order[:1]))
    backward = [(b, a) for a, b in onward]
    ahead = lambda x: lax.ppermute(x, "expert", onward)
    back = lambda x: lax.ppermute(x, "expert", backward)
    swap = lambda x: lax.ppermute(x, "tensor", [(0, 1), (1, 0)])
    dp_swap = lambda x: lax.ppermute(x, "dp", [(0, 1), (1, 0)])

    hidden_units = expert_down.shape[1]
    shared_units = 2 * shared_down.shape[1]
    stored = (
        expert_gate[0].T,
        expert_up[0].T,
        expert_down[0],
        jnp.swapaxes(shared_gate, 1, 2).reshape(shared_units, width),
        jnp.swapaxes(shared_up, 1, 2).reshape(shared_units, width),
        shared_down.reshape(shared_units, width),
    )
    inputs = (tokens, norm_gain[None, :], router.T, expert_ids.T, modality[None, :])
    lead = call(lead_body, shape((8, LANES), f32), (), 1, 2**34, MIB)
    own, *parts = call(
        lambda *refs: prologue_body(experts, *refs),
        (shape((count, width + side), bf16),)
        + (shape((quarter, width + side), bf16),) * 2
        + (shape((quarter, width), bf16),) * 2,
        (lead, *inputs),
        8,
        4 * MIB,
        MIB,
        [pltpu.VMEM((count, side), f32)],
    )
    other = dp_swap(own)
    weights = stored

    def pair_part(mine, theirs):
        rows = 2 * mine.shape[0]
        return call(
            lambda *refs: pair_body(experts, *refs),
            (shape((rows, columns), f32), shape((rows, columns), bf16)),
            (mine, theirs, *weights[:3]),
            16,
            6 * rows * width * hidden_units,
            6 * width * hidden_units,
            [pltpu.VMEM((rows, width + side), bf16)],
        )

    def far_part(mine, theirs):
        return call(
            lambda *refs: far_body(experts, *refs),
            (shape((count, columns), bf16), shape((hidden_units, count), bf16)),
            (mine, theirs, *weights[:3]),
            16,
            5 * count * width * hidden_units,
            6 * width * hidden_units,
            [pltpu.VMEM((count, width + side), bf16)],
        )

    def far_keep(hidden):
        return call(
            far_keep_body,
            shape((count, columns), f32),
            (hidden, weights[2]),
            16,
            count * width * hidden_units,
            width * hidden_units,
        )

    def own_part(own):
        return call(
            lambda *refs: own_body(experts, *refs),
            (shape((count, columns), f32),) * 2,
            (own, *weights[:3]),
            16,
            6 * count * width * hidden_units,
            6 * width * hidden_units,
        )

    def shared_part(*values):
        return call(
            lambda *refs: shared_body(experts, *refs),
            (shape((2 * count, columns), f32), shape((2 * count, columns), bf16)),
            (*values, *weights[3:]),
            16,
            12 * shared_units * count * width,
            6 * width * shared_units,
        )

    def sums(k, bases, *arrived):
        return call(
            lambda *refs: sum_body(bases, *refs),
            (shape((half, columns), bf16),) * len(bases),
            (keep[k], recv[k], *arrived),
            8,
        )

    def travel(pair):
        return ahead(pair[0]), back(pair[1])

    def packed(pieces):
        rows = len(pieces) * pieces[0].shape[0]
        return call(
            lambda *refs: pack_body(width, *refs),
            shape((rows, width + side), bf16), pieces, 4,
        )

    keep, recv = {}, {}
    own_sums = own_part(own)
    long, short = parts[:2], parts[2:]
    for k in range(1, middle + 1):
        long = travel(long)
        if k < middle:
            short = travel(short)
            mine = packed((long[0], short[0], short[1], long[1]))
            keep[k], give = pair_part(mine, swap(mine))
        else:
            mine = packed(long)
            give, hidden = far_part(mine, swap(mine))
            keep[k] = far_keep(hidden)
        recv[k] = swap(give)

    ahead_base, back_base = count, 0
    short = sums(middle - 1, (ahead_base + half, back_base))
    long = call(far_add_body, (shape((half, columns), bf16),) * 2, (keep[middle], recv[middle]), 8)

    for k in range(middle - 1, 0, -1):
        long = travel(long)
        short = travel(short)
        if k > 1:
            for way, base in enumerate((ahead_base + half, back_base)):
                part = sums(k - 1, (base,), short[way])
                short = (*part, short[1]) if way == 0 else (short[0], *part)
        for way, base in enumerate((ahead_base, back_base + half)):
            part = sums(k, (base,), long[way])
            long = (*part, long[1]) if way == 0 else (long[0], *part)
    long = travel(long)

    local, give = shared_part(own, other, *own_sums)
    local = local + swap(give).astype(f32)
    local_other = dp_swap(local[count:].astype(bf16))
    return call(
        total_body,
        shape((count, columns), bf16),
        (local, local_other, long[0], short[0], short[1], long[1]),
        8,
    )


def solution(mesh):
    in_specs = (
        P(("dp", "expert"), None),
        P(),
        P(),
        P(("dp", "expert"), None),
        P(("dp", "expert")),
        P("expert", None, "tensor"),
        P("expert", None, "tensor"),
        P("expert", "tensor", None),
        P(None, None, ("dp", "tensor")),
        P(None, None, ("dp", "tensor")),
        P(None, ("dp", "tensor"), None),
    )
    out_specs = P(("dp", "expert"), "tensor")

    return jax.shard_map(
        per_device, mesh=mesh, in_specs=in_specs, out_specs=out_specs, check_vma=False
    )
```
